256 devices in a mesh: chol: 32 (over z_hi, y, x), virt: 8 (over z_lo, core).
Axes of the slice: x: 4, y: 4, z: 8 (z_hi: 2, z_lo: 4; z = z_hi * 4 + z_lo), core: 2. Of those that a mesh axis runs over, the one named last changes fastest.
Arguments:
- amplitudes: bfloat16 [9600, 600], P('chol'), may hold values from -6 to 6
- chol_vectors: bfloat16 [256, 600, 600], P('chol', 'virt'), may hold values from -0.061035156 to 0.061035156
Outputs:
- sigma: float32 [9600, 600], P('chol', 'virt')
The draws below stay inside these ranges and needn't reach their ends.
All inputs are finite; a program needn't handle non-finite values.
Results may differ from the reference program's by a relative error of at most 0.0042.
Values may be sent and summed in bfloat16 or wider, within the bound.
A program may use at most 128 MiB of HBM per device.

```python
import jax
import jax.numpy as jnp
from jax import lax

V = 600
ROOTS = 2
PAIRS = 8
CH_DEV = 8
NP = 256
N_CHOL = 32


def levels(rng, dims, split, least, high):
    def one(axis_at, parts):
        steps = jax.random.uniform(jax.random.fold_in(jax.random.fold_in(rng, 6), axis_at), (parts,), jnp.float32, least / len(split), high / len(split))
        return jnp.repeat(jnp.exp(steps), dims[axis_at] // parts).reshape((-1,) + (1,) * (len(dims) - axis_at - 1))

    gain = one(*split[0])
    for cut in split[1:]:
        gain = gain * one(*cut)
    return gain


def scatter_about(key, shape, deviation, reach, shards=(), dtype=jnp.bfloat16):
    values = deviation * jax.random.normal(key, shape, jnp.float32)
    if shards:
        values = values * levels(key, shape, shards, -0.22, 0.18)
    return jnp.clip(values, -reach, reach).astype(dtype)


def setup_inputs(seed: int = 0) -> dict:
    streams_of = jax.random.split(jax.random.key(seed), 3)
    return {
        "amplitudes": scatter_about(streams_of[0], (ROOTS * PAIRS * V, V), 1.0, 6.0, ((0, 32),)),
        "chol_vectors": scatter_about(streams_of[1], (NP, V, V), ((V * (CH_DEV * N_CHOL) ** 0.5) ** -0.5), 0.061035156, ((0, 32), (1, 8))),
    }


def reference(amplitudes, chol_vectors):
    combos = ROOTS * PAIRS

    def one_vector(running, vector):
        ladder_half = jnp.dot(amplitudes, vector.T, preferred_element_type=jnp.float32).astype(jnp.bfloat16)
        ladder_half = ladder_half.reshape(combos, V, V)
        update = jnp.einsum('ac,ncb->nab', vector.astype(jnp.float32), ladder_half.astype(jnp.float32), precision=lax.Precision.HIGHEST)
        return running + update, None

    zeros_init = jnp.zeros((combos, V, V), jnp.float32)
    total, unused = lax.scan(one_vector, zeros_init, chol_vectors)
    return total.reshape(combos * V, V)
```

```python
import jax
import jax.numpy as jnp
from jax import lax
from jax.experimental import pallas as pl
from jax.experimental.pallas import tpu as pltpu
from jax.sharding import PartitionSpec as P

BF, F32 = jnp.bfloat16, jnp.float32
MESH = pl.DeviceIdType.MESH
NT = (((1,), (1,)), ((), ()))
V, W = 600, 640
TB, TW = 300, 304
LB, LW = 75, 80
SW = 320
N_SEND = 160


def kernel(t_in, l_in, out, lr, rb, lk, tb, tn, h, acc, sb,
           rxb1, rxb2, rya1, rya2, ryb1, ryb2, rxa1, rxa2, fin, zs, zr,
           send_sem, l_sem, rb_sem, t_sem, rxb_sem, rya_sem, ryb_sem, rxa_sem, z_sem):
    ci, vj = lax.axis_index("chol"), lax.axis_index("virt")
    zh, y, x = ci // 16, (ci // 4) % 4, ci % 4
    zl, core = vj // 2, vj % 2
    xp, xf, xm = (x + 1) % 4, (x + 2) % 4, (x + 3) % 4
    yp, ym = (y + 1) % 4, (y + 3) % 4
    end = jnp.logical_or(zl == 0, zl == 3)
    mid = jnp.logical_not(end)
    cls = y % 2 == core
    non = jnp.logical_not(cls)
    nh = jnp.where(end, 1 - zh, zh)
    ph = zl // 2
    d2 = jnp.where(zl < 2, 2, -2)
    yi, ip, im = y // 2, yp // 2, ym // 2

    def dev(chol, virt):
        return {"chol": chol, "virt": virt}

    def dev_x(v):
        return dev(zh * 16 + y * 4 + v, vj)

    def dev_y(v):
        return dev(zh * 16 + v * 4 + x, vj)

    partner = dev(ci, vj + 1 - 2 * core)

    barrier = pltpu.get_barrier_semaphore()
    spot = zh * 8 + vj
    for o in range(1, 16):
        other = (spot + o) % 16
        pl.semaphore_signal(barrier, inc=1, device_id=dev((other // 8) * 16 + y * 4 + x, other % 8), device_id_type=MESH)
    for there in (dev_x(xp), dev_x(xm), dev_y(yp), dev_y(ym)):
        pl.semaphore_signal(barrier, inc=1, device_id=there, device_id_type=MESH)
    pl.semaphore_wait(barrier, 19)

    pending = []

    def when(cond, work):
        if cond is None:
            work()
        else:
            pl.when(cond)(work)

    def send(cond, src, dst, sem, there):
        copy = pltpu.make_async_remote_copy(
            src_ref=src, dst_ref=dst, send_sem=send_sem.at[len(pending)], recv_sem=sem,
            device_id=there, device_id_type=MESH)
        pending.append((cond, copy))
        when(cond, copy.start)

    def arrived(cond, region, sem):
        when(cond, pltpu.make_async_copy(region, region, sem).wait)

    def own_l(half, pair):
        return l_in.at[pl.ds(half * 4 + pair * 2, 2)]

    def l_at(pair, j):
        return lr.at[pair, :, j]

    up, down = dev(ci, (vj + d2) % 8), dev(ci, (vj - d2 + 8) % 8)
    j1, j2, j3 = (vj + d2 + 8) % 8, (vj + 2 * d2 + 8) % 8, (vj + 3 * d2 + 8) % 8
    je = (vj - d2 + 8) % 8

    def l_first(pair):
        send(end, own_l(1 - ph, pair), rb.at[pair], rb_sem.at[pair], up)
        send(mid, own_l(1 - ph, pair), l_at(pair, vj), l_sem.at[pair, vj], up)
        send(mid, own_l(ph, pair), l_at(pair, vj), l_sem.at[pair, vj], down)
        send(end, own_l(ph, pair), l_at(pair, vj), l_sem.at[pair, vj], up)

    def l_own(pair):
        send(None, own_l(ph, pair), l_at(pair, vj), l_sem.at[pair, vj], partner)
        pltpu.make_async_copy(own_l(ph, pair), l_at(pair, vj), l_sem.at[pair, vj]).start()

    def l_arrived(cond, pair, j):
        arrived(cond, l_at(pair, j), l_sem.at[pair, j])

    def l_pass(cond, pair, j, there):
        send(cond, l_at(pair, j), l_at(pair, j), l_sem.at[pair, j], there)

    def l_relay_end(pair):
        arrived(mid, rb.at[pair], rb_sem.at[pair])
        send(mid, rb.at[pair], l_at(pair, je), l_sem.at[pair, je], up)

    def l_relay_across(pair, j):
        l_arrived(mid, pair, j)
        l_pass(mid, pair, j, down)
        l_pass(mid, pair, j, partner)

    def l_share(cond, pair, j):
        l_arrived(cond, pair, j)
        l_pass(cond, pair, j, partner)

    A, A0, A1 = pl.ds(0, 160), pl.ds(0, 80), pl.ds(80, 80)
    B, B0, B1 = pl.ds(160, 144), pl.ds(160, 80), pl.ds(240, 64)

    def t_send(cond, i, xs, rows, kind, there):
        send(cond, tb.at[i, xs, rows], tb.at[i, xs, rows], t_sem.at[i, xs, kind], there)

    def t_arrived(cond, i, xs, rows, kind):
        arrived(cond, tb.at[i, xs, rows], t_sem.at[i, xs, kind])

    border = dev((1 - zh) * 16 + y * 4 + x, (3 - zl) * 2 + core)
    end_cls, mid_cls = jnp.logical_and(end, cls), jnp.logical_and(mid, cls)
    for rows, kind in ((B, 2), (A, 0)):
        send(end_cls, t_in.at[rows], tb.at[yi, x, rows], t_sem.at[yi, x, kind], border)
        when(mid_cls, pltpu.make_async_copy(t_in.at[rows], tb.at[yi, x, rows], t_sem.at[yi, x, kind]).start)
    l_first(0)
    l_first(1)
    t_arrived(cls, yi, x, B, 2)
    t_arrived(cls, yi, x, A, 0)
    for v in (xp, xm):
        t_send(cls, yi, x, A, 0, dev_x(v))
    for v in (yp, ym):
        t_send(cls, yi, x, B, 2, dev_y(v))
    for v in (xp, xm):
        t_send(cls, yi, x, B, 2, dev_x(v))
    for v in (yp, ym):
        t_send(cls, yi, x, A, 0, dev_y(v))
    l_own(0)
    l_own(1)
    tn[:, V:, :] = jnp.zeros((4, W - V, W), BF)

    t_arrived(non, im, x, B, 2)
    t_arrived(non, ip, x, B, 2)
    t_send(non, im, x, B0, 2, dev_y(yp))
    t_send(non, ip, x, B1, 3, dev_y(ym))
    for i in (im, ip):
        for v in (xp, xm):
            t_send(non, i, x, B, 2, dev_x(v))
    t_arrived(cls, yi, xm, A, 0)
    t_arrived(cls, yi, xp, A, 0)
    t_send(cls, yi, xm, A0, 0, dev_x(xp))
    t_send(cls, yi, xp, A1, 1, dev_x(xm))
    for xs in (xm, xp):
        for v in (yp, ym):
            t_send(cls, yi, xs, A, 0, dev_y(v))
    l_relay_end(0)
    l_relay_across(0, j1)
    l_share(end, 0, j1)
    t_arrived(cls, 1 - yi, x, B0, 2)
    t_arrived(cls, 1 - yi, x, B1, 3)
    for v in (xp, xm):
        t_send(cls, 1 - yi, x, B, 2, dev_x(v))
    t_arrived(cls, yi, xf, A0, 0)
    t_arrived(cls, yi, xf, A1, 1)
    for v in (yp, ym):
        t_send(cls, yi, xf, A, 0, dev_y(v))

    def a4(xs):
        t_arrived(non, im, xs, A, 0)
        t_arrived(non, ip, xs, A, 0)
        t_send(non, im, xs, A0, 0, dev_y(yp))
        t_send(non, ip, xs, A1, 1, dev_y(ym))

    def b4(i):
        t_arrived(None, i, xm, B, 2)
        t_arrived(None, i, xp, B, 2)
        t_send(None, i, xm, B0, 2, dev_x(xp))
        t_send(None, i, xp, B1, 3, dev_x(xm))

    a4(x)
    b4(yi)
    l_share(mid, 0, je)
    l_relay_across(1, j1)
    l_share(end, 1, j1)
    a4(xm)
    a4(xp)
    b4(1 - yi)
    l_relay_across(0, j2)
    l_relay_end(1)
    a4(xf)
    l_share(end, 0, j2)
    for i in (0, 1):
        t_arrived(None, i, xf, B0, 2)
        t_arrived(None, i, xf, B1, 3)
    for xs in range(4):
        t_arrived(cls, 1 - yi, xs, A0, 0)
        t_arrived(cls, 1 - yi, xs, A1, 1)
    l_share(mid, 1, je)
    l_relay_across(1, j2)
    l_share(end, 0, j3)

    for n in range(4):
        i, k = n // 2, 2 * (n % 2)
        tn[n, 0:TB, :] = tb[i, k, 0:TB, :]
        tn[n, TB:V, :] = tb[i, k + 1, 0:TB, :]

    l_own_j = [2 * s + 1 - core for s in range(4)]
    for pair in (0,):
        l_arrived(None, pair, vj)
        for j in l_own_j:
            l_arrived(None, pair, j)

    def lay(pair):
        both = lr[pair].reshape(2, W, W)
        lk[:, :W] = both[0]
        lk[:, W:] = both[1]

    def halves(pair, n0, n1):
        for k, n in enumerate((n0, n1)):
            half = lax.dot_general(tn[n], lr[pair].reshape(2 * W, W), NT, preferred_element_type=F32).astype(BF)
            h[:W, k * W:(k + 1) * W] = half[:, :W]
            h[W:, k * W:(k + 1) * W] = half[:, W:]
        return jnp.dot(lk[...], h[...], preferred_element_type=F32)

    lay(0)

    def first(g, carry):
        acc[g] = halves(0, 2 * g, 2 * g + 1)
        return carry

    lax.fori_loop(0, 2, first, 0)
    l_share(end, 1, j2)
    l_share(end, 1, j3)
    l_arrived(None, 1, vj)
    for j in l_own_j:
        l_arrived(None, 1, j)
    lay(1)

    def second(g, carry):
        total = acc[g] + halves(1, 2 * g, 2 * g + 1)
        for k in range(2):
            block = total[:, k * W:(k + 1) * W].astype(BF)
            sb[g, 2 * k] = block[:SW]
            sb[g, 2 * k + 1] = block[SW:]
        return carry

    lax.fori_loop(0, 2, second, 0)

    A, A0, A1 = pl.ds(0, 160), pl.ds(0, 80), pl.ds(80, 80)
    B, B0, B1 = pl.ds(160, 160), pl.ds(160, 80), pl.ds(240, 80)

    def add(i, xs, rows, *others):
        total = sb[i, xs, rows, :].astype(F32)
        for other in others:
            total = total + other[...].astype(F32)
        return total

    def put(cond, i, xs, rows, *others):
        def work():
            sb[i, xs, rows, :] = add(i, xs, rows, *others).astype(BF)
        when(cond, work)

    for i in (0, 1):
        send(None, sb.at[i, xf, B0], rxb1.at[0, i], rxb_sem.at[0, 0, i], dev_x(xp))
        send(None, sb.at[i, xf, B1], rxb1.at[1, i], rxb_sem.at[0, 1, i], dev_x(xm))
    for xs in range(4):
        send(cls, sb.at[1 - yi, xs, A0], rya1.at[0, xs], rya_sem.at[0, 0, xs], dev_y(yp))
        send(cls, sb.at[1 - yi, xs, A1], rya1.at[1, xs], rya_sem.at[0, 1, xs], dev_y(ym))
    for i in (0, 1):
        arrived(None, rxb1.at[0, i], rxb_sem.at[0, 0, i])
        put(None, i, xp, B0, rxb1.at[0, i])
        send(None, sb.at[i, xp, B], rxb2.at[0, i], rxb_sem.at[1, 0, i], dev_x(xp))
        arrived(None, rxb1.at[1, i], rxb_sem.at[0, 1, i])
        put(None, i, xm, B1, rxb1.at[1, i])
        send(None, sb.at[i, xm, B], rxb2.at[1, i], rxb_sem.at[1, 1, i], dev_x(xm))
    for xs in range(4):
        arrived(non, rya1.at[0, xs], rya_sem.at[0, 0, xs])
        put(non, ip, xs, A0, rya1.at[0, xs])
        send(non, sb.at[ip, xs, A], rya2.at[0, xs], rya_sem.at[1, 0, xs], dev_y(yp))
        arrived(non, rya1.at[1, xs], rya_sem.at[0, 1, xs])
        put(non, im, xs, A1, rya1.at[1, xs])
        send(non, sb.at[im, xs, A], rya2.at[1, xs], rya_sem.at[1, 1, xs], dev_y(ym))
    for i in (0, 1):
        arrived(None, rxb2.at[0, i], rxb_sem.at[1, 0, i])
        arrived(None, rxb2.at[1, i], rxb_sem.at[1, 1, i])
        put(None, i, x, B, rxb2.at[0, i], rxb2.at[1, i])
    send(cls, sb.at[1 - yi, x, B0], ryb1.at[0], ryb_sem.at[0, 0], dev_y(yp))
    send(cls, sb.at[1 - yi, x, B1], ryb1.at[1], ryb_sem.at[0, 1], dev_y(ym))
    for xs in range(4):
        arrived(cls, rya2.at[0, xs], rya_sem.at[1, 0, xs])
        arrived(cls, rya2.at[1, xs], rya_sem.at[1, 1, xs])
        put(cls, yi, xs, A, rya2.at[0, xs], rya2.at[1, xs])
    send(cls, sb.at[yi, xf, A0], rxa1.at[0], rxa_sem.at[0, 0], dev_x(xp))
    send(cls, sb.at[yi, xf, A1], rxa1.at[1], rxa_sem.at[0, 1], dev_x(xm))
    arrived(non, ryb1.at[0], ryb_sem.at[0, 0])
    put(non, ip, x, B0, ryb1.at[0])
    send(non, sb.at[ip, x, B], ryb2.at[0], ryb_sem.at[1, 0], dev_y(yp))
    arrived(non, ryb1.at[1], ryb_sem.at[0, 1])
    put(non, im, x, B1, ryb1.at[1])
    send(non, sb.at[im, x, B], ryb2.at[1], ryb_sem.at[1, 1], dev_y(ym))
    arrived(cls, rxa1.at[0], rxa_sem.at[0, 0])
    put(cls, yi, xp, A0, rxa1.at[0])
    send(cls, sb.at[yi, xp, A], rxa2.at[0], rxa_sem.at[1, 0], dev_x(xp))
    arrived(cls, rxa1.at[1], rxa_sem.at[0, 1])
    put(cls, yi, xm, A1, rxa1.at[1])
    send(cls, sb.at[yi, xm, A], rxa2.at[1], rxa_sem.at[1, 1], dev_x(xm))
    for k in range(2):
        arrived(cls, ryb2.at[k], ryb_sem.at[1, k])
        arrived(cls, rxa2.at[k], rxa_sem.at[1, k])

    @pl.when(cls)
    def _():
        fin[0:160, :] = add(yi, x, A, rxa2.at[0], rxa2.at[1])
        fin[160:320, :] = add(yi, x, B, ryb2.at[0], ryb2.at[1])
        fin[320:, :] = jnp.zeros((64, W), F32)
        zs[...] = fin[...].T.astype(BF).reshape(8, LW, 384)

    for o in (1, 2, 3, 4, 5, 6, 7):
        j = (vj + o) % 8
        send(cls, zs.at[j], zr.at[zl], z_sem.at[zl], dev(nh * 16 + y * 4 + x, j))
    send(end_cls, zs.at[vj], zr.at[zl], z_sem.at[zl], dev(nh * 16 + y * 4 + x, vj))
    when(mid_cls, pltpu.make_async_copy(zs.at[vj], zr.at[zl], z_sem.at[zl]).start)
    for s in range(4):
        arrived(None, zr.at[s], z_sem.at[s])
    total = zr[0].astype(F32) + zr[1].astype(F32) + zr[2].astype(F32) + zr[3].astype(F32)
    fin[0:LW, 0:384] = total
    turned = fin[0:128, 0:384].T
    for q in range(4):
        out[q * LB:(q + 1) * LB, :] = turned[q * LW:q * LW + LB, :LB]

    for cond, copy in pending:
        when(cond, copy.wait_send)


def shards(amplitudes, chol_vectors):
    t_in = jnp.pad(amplitudes, ((0, TW - TB), (0, W - V)))
    l_in = jnp.pad(chol_vectors, ((0, 0), (0, LW - LB), (0, W - V)))
    dma = pltpu.SemaphoreType.DMA
    vmem = pltpu.VMEM
    return pl.pallas_call(
        kernel,
        out_shape=jax.ShapeDtypeStruct((TB, LB), F32),
        in_specs=[pl.BlockSpec(memory_space=pltpu.VMEM)] * 2,
        out_specs=pl.BlockSpec(memory_space=pltpu.VMEM),
        scratch_shapes=[
            vmem((2, 2, 8, LW, W), BF), vmem((2, 2, LW, W), BF), vmem((W, 2 * W), BF),
            vmem((2, 4, TW, W), BF), vmem((4, W, W), BF), vmem((2 * W, 2 * W), BF),
            vmem((2, W, 2 * W), F32), vmem((2, 4, SW, W), BF),
            vmem((2, 2, 80, W), BF), vmem((2, 2, 160, W), BF),
            vmem((2, 4, 80, W), BF), vmem((2, 4, 160, W), BF),
            vmem((2, 80, W), BF), vmem((2, 160, W), BF), vmem((2, 80, W), BF), vmem((2, 160, W), BF),
            vmem((384, W), F32), vmem((8, LW, 384), BF), vmem((4, LW, 384), BF),
            dma((N_SEND,)), dma((2, 8)), dma((2,)), dma((2, 4, 4)),
            dma((2, 2, 2)), dma((2, 2, 4)), dma((2, 2)), dma((2, 2)), dma((4,)),
        ],
        compiler_params=pltpu.CompilerParams(
            collective_id=0, has_side_effects=True, vmem_limit_bytes=60 << 20),
        name="ladder",
    )(t_in, l_in)


def solution(mesh):
    placed = (P("chol", None), P("chol", "virt", None))
    return jax.shard_map(
        shards, mesh=mesh, in_specs=placed, out_specs=P("chol", "virt"), check_vma=False
    )
```

```python
import jax
import jax.numpy as jnp
from jax import lax
from jax.experimental import pallas as pl
from jax.experimental.pallas import tpu as pltpu
from jax.sharding import PartitionSpec as P

BF, F32 = jnp.bfloat16, jnp.float32
MESH = pl.DeviceIdType.MESH
NT = (((1,), (1,)), ((), ()))
V, W = 600, 640
TB, TW = 300, 304
LB, LW = 75, 80
SW = 320
N_SEND = 110


def kernel(t_raw, l_raw, out, t_in, l_in, lr, rb, lk, tb, tn, h, acc, sb,
           rxb1, rxb2, rya1, rya2, ryb1, ryb2, rxa1, rxa2, fin, zs, zr,
           send_sem, l_sem, rb_sem, t_sem, rxb_sem, rya_sem, ryb_sem, rxa_sem, z_sem, line_sem):
    ci, vj = lax.axis_index("chol"), lax.axis_index("virt")
    zh, y, x = ci // 16, (ci // 4) % 4, ci % 4
    zl, core = vj // 2, vj % 2
    xp, xf, xm = (x + 1) % 4, (x + 2) % 4, (x + 3) % 4
    yp, ym = (y + 1) % 4, (y + 3) % 4
    end = jnp.logical_or(zl == 0, zl == 3)
    mid = jnp.logical_not(end)
    cls = y % 2 == core
    non = jnp.logical_not(cls)
    nh = jnp.where(end, 1 - zh, zh)
    ph = zl // 2
    d2 = jnp.where(zl < 2, 2, -2)
    yi, ip, im = y // 2, yp // 2, ym // 2
    yf = (y + 2) % 4

    def row_of(g, xs):
        return (xs // 2 + g) % 2

    def cols_of(g, i):
        first_col = 2 * ((i + g) % 2)
        return first_col, first_col + 1

    def both(a, b):
        return jnp.logical_and(a, b)

    g_own = (x // 2 + yi) % 2
    g_near = jnp.where(end, 1, 0)
    g_far = 1 - g_near
    z_owner = (nh + g_own) % 2

    def dev(chol, virt):
        return {"chol": chol, "virt": virt}

    def dev_x(v):
        return dev(zh * 16 + y * 4 + v, vj)

    def dev_y(v):
        return dev(zh * 16 + v * 4 + x, vj)

    partner = dev(ci, vj + 1 - 2 * core)

    border = dev((1 - zh) * 16 + y * 4 + x, (3 - zl) * 2 + core)
    behind = dev((1 - zh) * 16 + y * 4 + x, (3 - zl) * 2 + core - d2)
    ahead = dev((1 - zh) * 16 + y * 4 + x, (3 - zl + d2 // 2) * 2 + core)
    up, down = dev(ci, (vj + d2) % 8), dev(ci, (vj - d2 + 8) % 8)

    barrier = pltpu.get_barrier_semaphore()
    for there in (dev_x(xp), dev_x(xm), dev_x(xf), dev_y(yp), dev_y(ym), dev_y(yf), up, partner):
        pl.semaphore_signal(barrier, inc=1, device_id=there, device_id_type=MESH)

    @pl.when(end)
    def _():
        pl.semaphore_signal(barrier, inc=1, device_id=border, device_id_type=MESH)
        pl.semaphore_signal(barrier, inc=1, device_id=behind, device_id_type=MESH)

    @pl.when(mid)
    def _():
        pl.semaphore_signal(barrier, inc=1, device_id=down, device_id_type=MESH)
        pl.semaphore_signal(barrier, inc=1, device_id=ahead, device_id_type=MESH)

    t_in[...] = jnp.zeros_like(t_in)
    t_in[:TB, :V] = t_raw[...]
    l_in[:, LB - 3:, :] = jnp.zeros((8, LW - LB + 3, W), BF)
    l_in[:, :, V - 88:] = jnp.zeros((8, LW, W - V + 88), BF)
    l_in[:, :LB, :V] = l_raw[...]
    tn[:, V:, :] = jnp.zeros((4, W - V, W), BF)
    pl.semaphore_wait(barrier, 10)

    pending = []

    def when(cond, work):
        if cond is None:
            work()
        else:
            pl.when(cond)(work)

    def send(cond, src, dst, sem, there):
        copy = pltpu.make_async_remote_copy(
            src_ref=src, dst_ref=dst, send_sem=send_sem.at[len(pending)], recv_sem=sem,
            device_id=there, device_id_type=MESH)
        pending.append((cond, copy.wait_send))
        when(cond, copy.start)

    def arrived(cond, region, sem):
        when(cond, pltpu.make_async_copy(region, region, sem).wait)

    def own_l(half, pair):
        return l_in.at[pl.ds(half * 4 + pair * 2, 2)]

    def l_at(pair, j):
        return lr.at[pair, :, j]

    j1, j2, j3 = (vj + d2 + 8) % 8, (vj + 2 * d2 + 8) % 8, (vj + 3 * d2 + 8) % 8
    je = (vj - d2 + 8) % 8

    def l_first(pair):
        send(end, own_l(1 - ph, pair), rb.at[pair], rb_sem.at[pair], up)
        send(mid, own_l(1 - ph, pair), l_at(pair, vj), l_sem.at[pair, vj], up)
        send(mid, own_l(ph, pair), l_at(pair, vj), l_sem.at[pair, vj], down)
        send(end, own_l(ph, pair), l_at(pair, vj), l_sem.at[pair, vj], up)

    def l_own(pair):
        send(None, own_l(ph, pair), l_at(pair, vj), l_sem.at[pair, vj], partner)
        pltpu.make_async_copy(own_l(ph, pair), l_at(pair, vj), l_sem.at[pair, vj]).start()

    def l_arrived(cond, pair, j):
        arrived(cond, l_at(pair, j), l_sem.at[pair, j])

    def l_pass(cond, pair, j, there):
        send(cond, l_at(pair, j), l_at(pair, j), l_sem.at[pair, j], there)

    def l_relay_end(pair):
        arrived(mid, rb.at[pair], rb_sem.at[pair])
        send(mid, rb.at[pair], l_at(pair, je), l_sem.at[pair, je], up)

    def l_relay_across(pair, j):
        l_arrived(mid, pair, j)
        l_pass(mid, pair, j, down)
        l_pass(mid, pair, j, partner)

    def l_share(cond, pair, j):
        l_arrived(cond, pair, j)
        l_pass(cond, pair, j, partner)

    A, B = pl.ds(0, 160), pl.ds(160, 144)
    own_near, own_far = both(cls, g_own == g_near), both(cls, g_own == g_far)

    def t_at(i, xs, rows):
        return tb.at[i, xs, rows], t_sem.at[i, xs, 0 if rows is A else 1]

    def t_send(cond, i, xs, rows, theres):
        region, sem = t_at(i, xs, rows)
        copies = [pltpu.make_async_remote_copy(
            src_ref=region, dst_ref=region, send_sem=send_sem.at[len(pending)], recv_sem=sem,
            device_id=there, device_id_type=MESH) for there in theres]

        def work():
            for copy in copies:
                copy.start()

        when(cond, work)
        three = tb.at[0, pl.ds(0, 3), rows]
        pending.append((cond, pltpu.make_async_copy(three, three, send_sem.at[len(pending)]).wait))

    def t_arrived(cond, i, xs, rows):
        arrived(cond, *t_at(i, xs, rows))

    x_others, y_others = [dev_x(v) for v in (xp, xm, xf)], [dev_y(v) for v in (yp, ym, yf)]
    end_cls = both(end, cls)

    def t_start():
        for rows in (A, B):
            region, sem = t_at(yi, x, rows)
            send(both(end_cls, g_own == 0), t_in.at[rows], region, sem, border)
            send(both(end_cls, g_own == 1), t_in.at[rows], region, sem, behind)
            when(own_near, pltpu.make_async_copy(t_in.at[rows], region, sem).start)

    def t_own(cond):
        t_arrived(cond, yi, x, A)
        t_send(cond, yi, x, A, x_others)
        t_arrived(cond, yi, x, B)
        t_send(cond, yi, x, B, y_others)
        t_send(cond, yi, x, B, x_others)
        t_send(cond, yi, x, A, y_others)

    def t_second(g):
        for xs in cols_of(g, yi):
            t_arrived(both(cls, xs != x), yi, xs, A)
            t_send(both(cls, xs != x), yi, xs, A, y_others)
        i = row_of(g, x)
        cond = jnp.logical_or(non, i != yi)
        t_arrived(cond, i, x, B)
        t_send(cond, i, x, B, x_others)

    def t_join(g):
        for i in (0, 1):
            for xs in cols_of(g, i):
                t_arrived(jnp.logical_or(non, yi != i), i, xs, A)
                t_arrived(xs != x, i, xs, B)
            n, k = (g, 2 * g) if i == 0 else (3 - g, 2 * (1 - g))
            tn[n, 0:TB, :] = tb[i, k, 0:TB, :]
            tn[n, TB:V, :] = tb[i, k + 1, 0:TB, :]

    t_start()
    l_first(0)
    l_first(1)
    t_own(own_near)
    l_own(0)
    l_own(1)
    l_relay_end(0)
    l_relay_across(0, j1)
    l_share(end, 0, j1)
    t_own(own_far)
    t_second(g_near)
    l_share(mid, 0, je)
    l_relay_across(1, j1)
    l_share(end, 1, j1)
    l_relay_across(0, j2)
    l_relay_end(1)
    t_second(g_far)
    l_share(end, 0, j2)
    l_share(mid, 1, je)
    l_relay_across(1, j2)
    l_share(end, 0, j3)
    t_join(g_near)
    partner_j = [2 * s + 1 - core for s in range(4)]
    l_arrived(None, 0, vj)
    for j in partner_j:
        l_arrived(None, 0, j)

    def lay(pair):
        both = lr[pair].reshape(2, W, W)
        lk[:, :W] = both[0]
        lk[:, W:] = both[1]

    def first_half(pair, k, n):
        half = lax.dot_general(tn[n], lr[pair].reshape(2 * W, W), NT, preferred_element_type=F32).astype(BF)
        h[:W, k * W:(k + 1) * W] = half[:, :W]
        h[W:, k * W:(k + 1) * W] = half[:, W:]

    def join_halves(pair, g):
        first_half(pair, 0, g)
        first_half(pair, 1, 3 - g)

    lay(0)
    join_halves(0, g_near)
    acc[0] = jnp.dot(lk[...], h[...], preferred_element_type=F32)
    l_share(end, 1, j2)
    t_join(g_far)
    join_halves(0, g_far)
    acc[1] = jnp.dot(lk[...], h[...], preferred_element_type=F32)
    l_share(end, 1, j3)
    l_arrived(None, 1, vj)
    for j in partner_j:
        l_arrived(None, 1, j)

    @pl.when(end)
    def _():
        pl.semaphore_signal(line_sem, inc=1, device_id=border, device_id_type=MESH)

    lay(1)

    def second(order, g):
        total = acc[order] + jnp.dot(lk[...], h[...], preferred_element_type=F32)
        for k, c in ((0, g), (1, 1 - g)):
            block = total[:, k * W:(k + 1) * W].astype(BF)
            sb[k, 2 * c] = block[:SW]
            sb[k, 2 * c + 1] = block[SW:]

    A, A0, A1 = pl.ds(0, 160), pl.ds(0, 80), pl.ds(80, 80)
    B, B0, B1 = pl.ds(160, 160), pl.ds(160, 80), pl.ds(240, 80)

    def add(i, xs, rows, *others):
        total = sb[i, xs, rows, :].astype(F32)
        for other in others:
            total = total + other[...].astype(F32)
        return total

    def put(cond, i, xs, rows, *others):
        def work():
            sb[i, xs, rows, :] = add(i, xs, rows, *others).astype(BF)
        when(cond, work)

    def r1(g):
        i = row_of(g, xf)
        send(None, sb.at[i, xf, B0], rxb1.at[0, i], rxb_sem.at[0, 0, i], dev_x(xp))
        send(None, sb.at[i, xf, B1], rxb1.at[1, i], rxb_sem.at[0, 1, i], dev_x(xm))
        for xs in cols_of(g, 1 - yi):
            send(cls, sb.at[1 - yi, xs, A0], rya1.at[0, xs], rya_sem.at[0, 0, xs], dev_y(yp))
            send(cls, sb.at[1 - yi, xs, A1], rya1.at[1, xs], rya_sem.at[0, 1, xs], dev_y(ym))

    def r2(g):
        i = row_of(g, xp)
        arrived(None, rxb1.at[0, i], rxb_sem.at[0, 0, i])
        put(None, i, xp, B0, rxb1.at[0, i])
        send(None, sb.at[i, xp, B], rxb2.at[0, i], rxb_sem.at[1, 0, i], dev_x(xp))
        i = row_of(g, xm)
        arrived(None, rxb1.at[1, i], rxb_sem.at[0, 1, i])
        put(None, i, xm, B1, rxb1.at[1, i])
        send(None, sb.at[i, xm, B], rxb2.at[1, i], rxb_sem.at[1, 1, i], dev_x(xm))
        for k in range(2):
            xs = cols_of(g, ip)[k]
            arrived(non, rya1.at[0, xs], rya_sem.at[0, 0, xs])
            put(non, ip, xs, A0, rya1.at[0, xs])
            send(non, sb.at[ip, xs, A], rya2.at[0, xs], rya_sem.at[1, 0, xs], dev_y(yp))
            xs = cols_of(g, im)[k]
            arrived(non, rya1.at[1, xs], rya_sem.at[0, 1, xs])
            put(non, im, xs, A1, rya1.at[1, xs])
            send(non, sb.at[im, xs, A], rya2.at[1, xs], rya_sem.at[1, 1, xs], dev_y(ym))

    def r3(g):
        i = row_of(g, x)
        arrived(None, rxb2.at[0, i], rxb_sem.at[1, 0, i])
        arrived(None, rxb2.at[1, i], rxb_sem.at[1, 1, i])
        put(None, i, x, B, rxb2.at[0, i], rxb2.at[1, i])
        far = both(cls, i != yi)
        send(far, sb.at[1 - yi, x, B0], ryb1.at[0], ryb_sem.at[0, 0], dev_y(yp))
        send(far, sb.at[1 - yi, x, B1], ryb1.at[1], ryb_sem.at[0, 1], dev_y(ym))
        for xs in cols_of(g, yi):
            arrived(cls, rya2.at[0, xs], rya_sem.at[1, 0, xs])
            arrived(cls, rya2.at[1, xs], rya_sem.at[1, 1, xs])
            put(cls, yi, xs, A, rya2.at[0, xs], rya2.at[1, xs])
        far = both(cls, row_of(g, xf) == yi)
        send(far, sb.at[yi, xf, A0], rxa1.at[0], rxa_sem.at[0, 0], dev_x(xp))
        send(far, sb.at[yi, xf, A1], rxa1.at[1], rxa_sem.at[0, 1], dev_x(xm))

    def r4(g):
        i = row_of(g, x)
        to_up, to_down = both(non, i == ip), both(non, i == im)
        arrived(to_up, ryb1.at[0], ryb_sem.at[0, 0])
        put(to_up, ip, x, B0, ryb1.at[0])
        send(to_up, sb.at[ip, x, B], ryb2.at[0], ryb_sem.at[1, 0], dev_y(yp))
        arrived(to_down, ryb1.at[1], ryb_sem.at[0, 1])
        put(to_down, im, x, B1, ryb1.at[1])
        send(to_down, sb.at[im, x, B], ryb2.at[1], ryb_sem.at[1, 1], dev_y(ym))
        to_up, to_down = both(cls, row_of(g, xp) == yi), both(cls, row_of(g, xm) == yi)
        arrived(to_up, rxa1.at[0], rxa_sem.at[0, 0])
        put(to_up, yi, xp, A0, rxa1.at[0])
        send(to_up, sb.at[yi, xp, A], rxa2.at[0], rxa_sem.at[1, 0], dev_x(xp))
        arrived(to_down, rxa1.at[1], rxa_sem.at[0, 1])
        put(to_down, yi, xm, A1, rxa1.at[1])
        send(to_down, sb.at[yi, xm, A], rxa2.at[1], rxa_sem.at[1, 1], dev_x(xm))

    join_halves(1, g_near)
    second(0, g_near)
    r1(g_near)
    join_halves(1, g_far)
    r2(g_near)
    second(1, g_far)
    r1(g_far)
    r3(g_near)
    r2(g_far)
    pl.semaphore_wait(line_sem, 1)

    @pl.when(end)
    def _():
        pl.semaphore_signal(line_sem, inc=1, device_id=up, device_id_type=MESH)

    r4(g_near)
    r3(g_far)
    r4(g_far)
    for k in range(2):
        arrived(cls, ryb2.at[k], ryb_sem.at[1, k])
        arrived(cls, rxa2.at[k], rxa_sem.at[1, k])

    @pl.when(cls)
    def _():
        fin[0:160, :] = add(yi, x, A, rxa2.at[0], rxa2.at[1])
        fin[160:320, :] = add(yi, x, B, ryb2.at[0], ryb2.at[1])
        fin[320:, :] = jnp.zeros((64, W), F32)
        zs[...] = fin[...].T.astype(BF).reshape(8, LW, 384)

    away = z_owner != zh
    for o in range(8):
        j = (vj + o) % 8
        send(both(cls, away) if o == 0 else cls, zs.at[j], zr.at[zl], z_sem.at[zl], dev(z_owner * 16 + y * 4 + x, j))
    when(both(cls, z_owner == zh), pltpu.make_async_copy(zs.at[vj], zr.at[zl], z_sem.at[zl]).start)
    for s in range(4):
        arrived(None, zr.at[s], z_sem.at[s])
    total = zr[0].astype(F32) + zr[1].astype(F32) + zr[2].astype(F32) + zr[3].astype(F32)
    for q in range(4):
        out[:, q * LB:(q + 1) * LB] = total[:LB, q * LW:q * LW + LB]

    assert len(pending) <= N_SEND, len(pending)
    for cond, wait in pending:
        when(cond, wait)


def shards(amplitudes, chol_vectors):
    dma = pltpu.SemaphoreType.DMA
    vmem = pltpu.VMEM
    turned = pl.pallas_call(
        kernel,
        out_shape=jax.ShapeDtypeStruct((LB, TB), F32),
        in_specs=[pl.BlockSpec(memory_space=pltpu.VMEM)] * 2,
        out_specs=pl.BlockSpec(memory_space=pltpu.VMEM),
        scratch_shapes=[
            vmem((TW, W), BF), vmem((8, LW, W), BF),
            vmem((2, 2, 8, LW, W), BF), vmem((2, 2, LW, W), BF), vmem((W, 2 * W), BF),
            vmem((2, 4, TW, W), BF), vmem((4, W, W), BF), vmem((2 * W, 2 * W), BF),
            vmem((2, W, 2 * W), F32), vmem((2, 4, SW, W), BF),
            vmem((2, 2, 80, W), BF), vmem((2, 2, 160, W), BF),
            vmem((2, 4, 80, W), BF), vmem((2, 4, 160, W), BF),
            vmem((2, 80, W), BF), vmem((2, 160, W), BF), vmem((2, 80, W), BF), vmem((2, 160, W), BF),
            vmem((384, W), F32), vmem((8, LW, 384), BF), vmem((4, LW, 384), BF),
            dma((N_SEND,)), dma((2, 8)), dma((2,)), dma((2, 4, 2)),
            dma((2, 2, 2)), dma((2, 2, 4)), dma((2, 2)), dma((2, 2)), dma((4,)),
            pltpu.SemaphoreType.REGULAR,
        ],
        compiler_params=pltpu.CompilerParams(
            collective_id=0, has_side_effects=True, vmem_limit_bytes=52 << 20),
        name="ladder",
    )(amplitudes, chol_vectors)
    return turned.T


def solution(mesh):
    placed = (P("chol", None), P("chol", "virt", None))
    return jax.shard_map(
        shards, mesh=mesh, in_specs=placed, out_specs=P("chol", "virt"), check_vma=False
    )
```

```python
import jax
import jax.numpy as jnp
from jax import lax
from jax.experimental import pallas as pl
from jax.experimental.pallas import tpu as pltpu
from jax.sharding import PartitionSpec as P

BF, F32 = jnp.bfloat16, jnp.float32
MESH = pl.DeviceIdType.MESH
NT = (((1,), (1,)), ((), ()))
V, W = 600, 640
TB, TW = 300, 304
LB, LW = 75, 80
SW = 320
N_SEND = 84


def kernel(t_raw, l_raw, out, t_in, l_in, lr, lk, tb, tn, h, acc, sb,
           rxb, rya, ryb, rxa, fin, zs, zr,
           send_sem, l_sem, t_sem, rxb_sem, rya_sem, ryb_sem, rxa_sem, z_sem, line_sem):
    ci, vj = lax.axis_index("chol"), lax.axis_index("virt")
    zh, y, x = ci // 16, (ci // 4) % 4, ci % 4
    zl, core = vj // 2, vj % 2
    xp, xf, xm = (x + 1) % 4, (x + 2) % 4, (x + 3) % 4
    yp, ym = (y + 1) % 4, (y + 3) % 4
    end = jnp.logical_or(zl == 0, zl == 3)
    mid = jnp.logical_not(end)
    cls = y % 2 == core
    non = jnp.logical_not(cls)
    nh = jnp.where(end, 1 - zh, zh)
    ph = zl // 2
    d2 = jnp.where(zl < 2, 2, -2)
    yi, ip, im = y // 2, yp // 2, ym // 2
    yf = (y + 2) % 4

    def row_of(g, xs):
        return (xs // 2 + g) % 2

    def cols_of(g, i):
        first_col = 2 * ((i + g) % 2)
        return first_col, first_col + 1

    def both(a, b):
        return jnp.logical_and(a, b)

    g_own = (x // 2 + yi) % 2
    g_near = jnp.where(end, 1, 0)
    g_far = 1 - g_near
    z_owner = (nh + g_own) % 2

    def dev(chol, virt):
        return {"chol": chol, "virt": virt}

    def dev_x(v):
        return dev(zh * 16 + y * 4 + v, vj)

    def dev_y(v):
        return dev(zh * 16 + v * 4 + x, vj)

    partner = dev(ci, vj + 1 - 2 * core)

    border = dev((1 - zh) * 16 + y * 4 + x, (3 - zl) * 2 + core)
    behind = dev((1 - zh) * 16 + y * 4 + x, (3 - zl) * 2 + core - d2)
    ahead = dev((1 - zh) * 16 + y * 4 + x, (3 - zl + d2 // 2) * 2 + core)
    up, down = dev(ci, (vj + d2) % 8), dev(ci, (vj - d2 + 8) % 8)

    opposite = dev(ci, (vj + 2 * d2 + 8) % 8)

    barrier = pltpu.get_barrier_semaphore()
    for there in (dev_x(xp), dev_x(xm), dev_x(xf), dev_y(yp), dev_y(ym), dev_y(yf), up, opposite, partner):
        pl.semaphore_signal(barrier, inc=1, device_id=there, device_id_type=MESH)

    @pl.when(end)
    def _():
        pl.semaphore_signal(barrier, inc=1, device_id=border, device_id_type=MESH)
        pl.semaphore_signal(barrier, inc=1, device_id=behind, device_id_type=MESH)

    @pl.when(mid)
    def _():
        pl.semaphore_signal(barrier, inc=1, device_id=down, device_id_type=MESH)
        pl.semaphore_signal(barrier, inc=1, device_id=ahead, device_id_type=MESH)

    t_in[...] = jnp.zeros_like(t_in)
    t_in[:TB, :V] = t_raw[...]
    l_in[:, LB - 3:, :] = jnp.zeros((8, LW - LB + 3, W), BF)
    l_in[:, :, V - 88:] = jnp.zeros((8, LW, W - V + 88), BF)
    l_in[:, :LB, :V] = l_raw[...]
    tn[:, V:, :] = jnp.zeros((4, W - V, W), BF)
    pl.semaphore_wait(barrier, 11)

    pending = []

    def when(cond, work):
        if cond is None:
            work()
        else:
            pl.when(cond)(work)

    def send(cond, src, dst, sem, there):
        copy = pltpu.make_async_remote_copy(
            src_ref=src, dst_ref=dst, send_sem=send_sem.at[len(pending)], recv_sem=sem,
            device_id=there, device_id_type=MESH)
        pending.append((cond, copy.wait_send))
        when(cond, copy.start)

    def arrived(cond, region, sem):
        when(cond, pltpu.make_async_copy(region, region, sem).wait)

    def own_l(half, pair):
        return l_in.at[pl.ds(half * 4 + pair * 2, 2)]

    def l_at(pair, j):
        return lr.at[pair, :, j]

    j1, j2, j3 = (vj + d2 + 8) % 8, (vj + 2 * d2 + 8) % 8, (vj + 3 * d2 + 8) % 8
    je = (vj - d2 + 8) % 8

    def l_first():
        send(mid, own_l(1 - ph, 0), l_at(0, vj), l_sem.at[0, vj], up)
        for pair in (0, 1):
            send(mid, own_l(ph, pair), l_at(pair, vj), l_sem.at[pair, vj], down)
            send(end, own_l(ph, pair), l_at(pair, vj), l_sem.at[pair, vj], up)
            send(end, own_l(1 - ph, pair), l_at(pair, vj), l_sem.at[pair, vj], opposite)

    def l_own(pair):
        send(None, own_l(ph, pair), l_at(pair, vj), l_sem.at[pair, vj], partner)
        pltpu.make_async_copy(own_l(ph, pair), l_at(pair, vj), l_sem.at[pair, vj]).start()

    def l_arrived(cond, pair, j):
        arrived(cond, l_at(pair, j), l_sem.at[pair, j])

    def l_pass(cond, pair, j, there):
        send(cond, l_at(pair, j), l_at(pair, j), l_sem.at[pair, j], there)

    def l_relay_across(pair, j):
        l_arrived(mid, pair, j)
        l_pass(mid, pair, j, down)
        l_pass(mid, pair, j, partner)

    def l_share(cond, pair, j):
        l_arrived(cond, pair, j)
        l_pass(cond, pair, j, partner)

    TA, TR = pl.ds(0, 160), pl.ds(160, 144)
    own_near, own_far = both(cls, g_own == g_near), both(cls, g_own == g_far)

    def t_at(i, xs, rows):
        return tb.at[i, xs, rows], t_sem.at[i, xs, 0 if rows is TA else 1]

    def t_send(cond, i, xs, rows, theres):
        region, sem = t_at(i, xs, rows)
        copies = [pltpu.make_async_remote_copy(
            src_ref=region, dst_ref=region, send_sem=send_sem.at[len(pending)], recv_sem=sem,
            device_id=there, device_id_type=MESH) for there in theres]

        def work():
            for copy in copies:
                copy.start()

        when(cond, work)
        three = tb.at[0, pl.ds(0, 3), rows]
        pending.append((cond, pltpu.make_async_copy(three, three, send_sem.at[len(pending)]).wait))

    def t_arrived(cond, i, xs, rows):
        arrived(cond, *t_at(i, xs, rows))

    x_others, y_others = [dev_x(v) for v in (xp, xm, xf)], [dev_y(v) for v in (yp, ym, yf)]
    end_cls = both(end, cls)

    def t_start():
        for rows in (TA, TR):
            region, sem = t_at(yi, x, rows)
            send(both(end_cls, g_own == 0), t_in.at[rows], region, sem, border)
            send(both(end_cls, g_own == 1), t_in.at[rows], region, sem, behind)
            when(own_near, pltpu.make_async_copy(t_in.at[rows], region, sem).start)

    def t_own(cond):
        t_arrived(cond, yi, x, TA)
        t_send(cond, yi, x, TA, x_others)
        t_arrived(cond, yi, x, TR)
        t_send(cond, yi, x, TR, y_others)
        t_send(cond, yi, x, TR, x_others)
        t_send(cond, yi, x, TA, y_others)

    def t_second(g):
        for xs in cols_of(g, yi):
            t_arrived(both(cls, xs != x), yi, xs, TA)
            t_send(both(cls, xs != x), yi, xs, TA, y_others)
        i = row_of(g, x)
        cond = jnp.logical_or(non, i != yi)
        t_arrived(cond, i, x, TR)
        t_send(cond, i, x, TR, x_others)

    def t_join(g):
        for i in (0, 1):
            for xs in cols_of(g, i):
                t_arrived(jnp.logical_or(non, yi != i), i, xs, TA)
                t_arrived(xs != x, i, xs, TR)
            n, k = (g, 2 * g) if i == 0 else (3 - g, 2 * (1 - g))
            tn[n, 0:TB, :] = tb[i, k, 0:TB, :]
            tn[n, TB:V, :] = tb[i, k + 1, 0:TB, :]

    t_start()
    l_first()
    t_own(own_near)
    l_own(0)
    l_own(1)
    l_relay_across(0, j1)
    send(mid, own_l(1 - ph, 1), l_at(1, vj), l_sem.at[1, vj], up)
    l_share(end, 0, j1)
    l_share(mid, 0, je)
    t_own(own_far)
    t_second(g_near)
    l_relay_across(0, j2)
    l_share(end, 1, j1)
    l_relay_across(1, j1)
    l_share(end, 0, j2)
    l_share(mid, 1, je)
    t_second(g_far)
    l_relay_across(1, j2)
    l_share(end, 0, j3)
    t_join(g_near)
    partner_j = [2 * s + 1 - core for s in range(4)]
    l_arrived(None, 0, vj)
    for j in partner_j:
        l_arrived(None, 0, j)

    def lay(pair):
        rows = lr[pair].reshape(2, W, W)
        lk[pair, :, :W] = rows[0]
        lk[pair, :, W:] = rows[1]

    def first_half(pair, k, n):
        half = lax.dot_general(tn[n], lr[pair].reshape(2 * W, W), NT, preferred_element_type=F32).astype(BF)
        h[:W, k * W:(k + 1) * W] = half[:, :W]
        h[W:, k * W:(k + 1) * W] = half[:, W:]

    def join_halves(pair, g):
        first_half(pair, 0, g)
        first_half(pair, 1, 3 - g)

    def first(g):
        join_halves(0, g)
        acc[...] = jnp.dot(lk[0], h[...], preferred_element_type=F32)

    def second(g):
        total = acc[...] + jnp.dot(lk[1], h[...], preferred_element_type=F32)
        for k, c in ((0, g), (1, 1 - g)):
            block = total[:, k * W:(k + 1) * W].astype(BF)
            sb[k, 2 * c] = block[:SW]
            sb[k, 2 * c + 1] = block[SW:]

    lay(0)
    first(g_near)
    l_share(end, 1, j2)
    l_share(end, 1, j3)
    l_arrived(None, 1, vj)
    for j in partner_j:
        l_arrived(None, 1, j)

    @pl.when(end)
    def _():
        pl.semaphore_signal(line_sem, inc=1, device_id=border, device_id_type=MESH)

    lay(1)
    join_halves(1, g_near)
    second(g_near)

    A, B = pl.ds(0, 160), pl.ds(160, 160)

    def add(i, xs, rows, *others):
        total = sb[i, xs, rows, :].astype(F32)
        for other in others:
            total = total + other[...].astype(F32)
        return total

    def put(cond, i, xs, rows, *others):
        def work():
            sb[i, xs, rows, :] = add(i, xs, rows, *others).astype(BF)
        when(cond, work)

    def large(g):
        for slot, v in enumerate((xp, xm, xf)):
            i = row_of(g, v)
            send(None, sb.at[i, v, B], rxb.at[slot, i], rxb_sem.at[slot, i], dev_x(v))
        for k in range(2):
            xs = cols_of(g, 1 - yi)[k]
            send(cls, sb.at[1 - yi, xs, A], rya.at[2, xs], rya_sem.at[2, xs], dev_y(yf))
            xs = cols_of(g, ip)[k]
            send(non, sb.at[ip, xs, A], rya.at[0, xs], rya_sem.at[0, xs], dev_y(yp))
            xs = cols_of(g, im)[k]
            send(non, sb.at[im, xs, A], rya.at[1, xs], rya_sem.at[1, xs], dev_y(ym))

    def small(g):
        i = row_of(g, x)
        for slot in range(3):
            arrived(None, rxb.at[slot, i], rxb_sem.at[slot, i])
        put(None, i, x, B, rxb.at[0, i], rxb.at[1, i], rxb.at[2, i])
        send(both(cls, yi != i), sb.at[i, x, B], ryb.at[2], ryb_sem.at[2], dev_y(yf))
        send(both(non, ip == i), sb.at[i, x, B], ryb.at[0], ryb_sem.at[0], dev_y(yp))
        send(both(non, im == i), sb.at[i, x, B], ryb.at[1], ryb_sem.at[1], dev_y(ym))
        for xs in cols_of(g, yi):
            for slot in range(3):
                arrived(cls, rya.at[slot, xs], rya_sem.at[slot, xs])
            put(cls, yi, xs, A, rya.at[0, xs], rya.at[1, xs], rya.at[2, xs])
        for slot, v in enumerate((xp, xm, xf)):
            send(both(cls, row_of(g, v) == yi), sb.at[yi, v, A], rxa.at[slot], rxa_sem.at[slot], dev_x(v))

    large(g_near)
    t_join(g_far)
    first(g_far)
    join_halves(1, g_far)
    second(g_far)
    large(g_far)
    small(g_near)
    pl.semaphore_wait(line_sem, 1)

    @pl.when(end)
    def _():
        pl.semaphore_signal(line_sem, inc=1, device_id=up, device_id_type=MESH)

    small(g_far)
    for slot in range(3):
        arrived(cls, ryb.at[slot], ryb_sem.at[slot])
        arrived(cls, rxa.at[slot], rxa_sem.at[slot])

    @pl.when(cls)
    def _():
        fin[0:160, :] = add(yi, x, A, rxa.at[0], rxa.at[1], rxa.at[2])
        fin[160:320, :] = add(yi, x, B, ryb.at[0], ryb.at[1], ryb.at[2])
        fin[320:, :] = jnp.zeros((64, W), F32)
        zs[...] = fin[...].T.astype(BF).reshape(8, LW, 384)

    away = z_owner != zh
    z_first = jnp.where((zl < 2) == away, 0, 3)
    z_step = jnp.where(z_first == 0, 1, -1)
    for o in range(4):
        for k in (0, 1):
            j = (z_first + o * z_step) * 2 + k
            send(both(cls, jnp.logical_or(away, j != vj)), zs.at[j], zr.at[zl], z_sem.at[zl],
                 dev(z_owner * 16 + y * 4 + x, j))
    when(both(cls, z_owner == zh), pltpu.make_async_copy(zs.at[vj], zr.at[zl], z_sem.at[zl]).start)
    for s in range(4):
        arrived(None, zr.at[s], z_sem.at[s])
    total = zr[0].astype(F32) + zr[1].astype(F32) + zr[2].astype(F32) + zr[3].astype(F32)
    for q in range(4):
        out[:, q * LB:(q + 1) * LB] = total[:LB, q * LW:q * LW + LB]

    assert len(pending) <= N_SEND, len(pending)
    for cond, wait in pending:
        when(cond, wait)


def shards(amplitudes, chol_vectors):
    dma = pltpu.SemaphoreType.DMA
    vmem = pltpu.VMEM
    turned = pl.pallas_call(
        kernel,
        out_shape=jax.ShapeDtypeStruct((LB, TB), F32),
        in_specs=[pl.BlockSpec(memory_space=pltpu.VMEM)] * 2,
        out_specs=pl.BlockSpec(memory_space=pltpu.VMEM),
        scratch_shapes=[
            vmem((TW, W), BF), vmem((8, LW, W), BF),
            vmem((2, 2, 8, LW, W), BF), vmem((2, W, 2 * W), BF),
            vmem((2, 4, TW, W), BF), vmem((4, W, W), BF), vmem((2 * W, 2 * W), BF),
            vmem((W, 2 * W), F32), vmem((2, 4, SW, W), BF),
            vmem((3, 2, 160, W), BF), vmem((3, 4, 160, W), BF), vmem((3, 160, W), BF), vmem((3, 160, W), BF),
            vmem((384, W), F32), vmem((8, LW, 384), BF), vmem((4, LW, 384), BF),
            dma((N_SEND,)), dma((2, 8)), dma((2, 4, 2)),
            dma((3, 2)), dma((3, 4)), dma((3,)), dma((3,)), dma((4,)),
            pltpu.SemaphoreType.REGULAR,
        ],
        compiler_params=pltpu.CompilerParams(
            collective_id=0, has_side_effects=True, vmem_limit_bytes=52 << 20),
        name="ladder",
    )(amplitudes, chol_vectors)
    return turned.T


def solution(mesh):
    placed = (P("chol", None), P("chol", "virt", None))
    return jax.shard_map(
        shards, mesh=mesh, in_specs=placed, out_specs=P("chol", "virt"), check_vma=False
    )
```

```python
import jax
import jax.numpy as jnp
from jax import lax
from jax.experimental import pallas as pl
from jax.experimental.pallas import tpu as pltpu
from jax.sharding import PartitionSpec as P

BF, F32 = jnp.bfloat16, jnp.float32
MESH = pl.DeviceIdType.MESH
NT = (((1,), (1,)), ((), ()))
V, W = 600, 640
TB, TW = 300, 304
LB, LW = 75, 80
SW = 320
N_SEND = 90


def kernel(t_raw, l_raw, out, t_in, l_in, lr, lk, tb, tn, h, acc, sb,
           rxb, rya, ryb, rxa, fin, zs, zr,
           send_sem, l_sem, t_sem, rxb_sem, rya_sem, ryb_sem, rxa_sem, z_sem, line_sem):
    ci, vj = lax.axis_index("chol"), lax.axis_index("virt")
    zh, y, x = ci // 16, (ci // 4) % 4, ci % 4
    zl, core = vj // 2, vj % 2
    xp, xf, xm = (x + 1) % 4, (x + 2) % 4, (x + 3) % 4
    yp, ym = (y + 1) % 4, (y + 3) % 4
    end = jnp.logical_or(zl == 0, zl == 3)
    mid = jnp.logical_not(end)
    cls = y % 2 == core
    non = jnp.logical_not(cls)
    nh = jnp.where(end, 1 - zh, zh)
    ph = zl // 2
    d2 = jnp.where(zl < 2, 2, -2)
    yi, ip, im = y // 2, yp // 2, ym // 2
    yf = (y + 2) % 4

    def row_of(g, xs):
        return (xs // 2 + g) % 2

    def cols_of(g, i):
        first_col = 2 * ((i + g) % 2)
        return first_col, first_col + 1

    def both(a, b):
        return jnp.logical_and(a, b)

    g_own = (x // 2 + yi) % 2
    g_near = jnp.where(end, 1, 0)
    g_far = 1 - g_near
    z_owner = (nh + g_own) % 2

    def dev(chol, virt):
        return {"chol": chol, "virt": virt}

    def dev_x(v):
        return dev(zh * 16 + y * 4 + v, vj)

    def dev_y(v):
        return dev(zh * 16 + v * 4 + x, vj)

    partner = dev(ci, vj + 1 - 2 * core)

    border = dev((1 - zh) * 16 + y * 4 + x, (3 - zl) * 2 + core)
    behind = dev((1 - zh) * 16 + y * 4 + x, (3 - zl) * 2 + core - d2)
    ahead = dev((1 - zh) * 16 + y * 4 + x, (3 - zl + d2 // 2) * 2 + core)
    up, down = dev(ci, (vj + d2) % 8), dev(ci, (vj - d2 + 8) % 8)

    opposite = dev(ci, (vj + 2 * d2 + 8) % 8)

    barrier = pltpu.get_barrier_semaphore()
    for there in (dev_x(xp), dev_x(xm), dev_x(xf), dev_y(yp), dev_y(ym), dev_y(yf), up, opposite, partner):
        pl.semaphore_signal(barrier, inc=1, device_id=there, device_id_type=MESH)

    @pl.when(end)
    def _():
        pl.semaphore_signal(barrier, inc=1, device_id=border, device_id_type=MESH)
        pl.semaphore_signal(barrier, inc=1, device_id=behind, device_id_type=MESH)

    @pl.when(mid)
    def _():
        pl.semaphore_signal(barrier, inc=1, device_id=down, device_id_type=MESH)
        pl.semaphore_signal(barrier, inc=1, device_id=ahead, device_id_type=MESH)

    t_in[...] = jnp.zeros_like(t_in)
    t_in[:TB, :V] = t_raw[...]
    l_in[:, LB - 3:, :] = jnp.zeros((8, LW - LB + 3, W), BF)
    l_in[:, :, V - 88:] = jnp.zeros((8, LW, W - V + 88), BF)
    l_in[:, :LB, :V] = l_raw[...]
    tn[:, V:, :] = jnp.zeros((4, W - V, W), BF)
    pl.semaphore_wait(barrier, 11)

    pending = []

    def when(cond, work):
        if cond is None:
            work()
        else:
            pl.when(cond)(work)

    def send(cond, src, dst, sem, there):
        copy = pltpu.make_async_remote_copy(
            src_ref=src, dst_ref=dst, send_sem=send_sem.at[len(pending)], recv_sem=sem,
            device_id=there, device_id_type=MESH)
        pending.append((cond, copy.wait_send))
        when(cond, copy.start)

    def arrived(cond, region, sem):
        when(cond, pltpu.make_async_copy(region, region, sem).wait)

    def own_l(half, pair):
        return l_in.at[pl.ds(half * 4 + pair * 2, 2)]

    def l_at(pair, j):
        return lr.at[pair, :, j]

    j1, j2, j3 = (vj + d2 + 8) % 8, (vj + 2 * d2 + 8) % 8, (vj + 3 * d2 + 8) % 8
    je = (vj - d2 + 8) % 8

    def l_first():
        send(mid, own_l(1 - ph, 0), l_at(0, vj), l_sem.at[0, vj], up)
        for pair in (0, 1):
            send(mid, own_l(ph, pair), l_at(pair, vj), l_sem.at[pair, vj], down)
            send(end, own_l(ph, pair), l_at(pair, vj), l_sem.at[pair, vj], up)
            send(end, own_l(1 - ph, pair), l_at(pair, vj), l_sem.at[pair, vj], opposite)

    def l_own(pair):
        send(None, own_l(ph, pair), l_at(pair, vj), l_sem.at[pair, vj], partner)
        pltpu.make_async_copy(own_l(ph, pair), l_at(pair, vj), l_sem.at[pair, vj]).start()

    def l_arrived(cond, pair, j):
        arrived(cond, l_at(pair, j), l_sem.at[pair, j])

    def l_pass(cond, pair, j, there):
        send(cond, l_at(pair, j), l_at(pair, j), l_sem.at[pair, j], there)

    def l_relay_across(pair, j):
        l_arrived(mid, pair, j)
        l_pass(mid, pair, j, down)
        l_pass(mid, pair, j, partner)

    def l_share(cond, pair, j):
        l_arrived(cond, pair, j)
        l_pass(cond, pair, j, partner)

    TA, TR = pl.ds(0, 160), pl.ds(160, 144)
    own_near, own_far = both(cls, g_own == g_near), both(cls, g_own == g_far)

    def t_at(i, xs, rows):
        return tb.at[i, xs, rows], t_sem.at[i, xs, 0 if rows is TA else 1]

    def t_send(cond, i, xs, rows, theres):
        region, sem = t_at(i, xs, rows)
        copies = [pltpu.make_async_remote_copy(
            src_ref=region, dst_ref=region, send_sem=send_sem.at[len(pending)], recv_sem=sem,
            device_id=there, device_id_type=MESH) for there in theres]

        def work():
            for copy in copies:
                copy.start()

        when(cond, work)
        three = tb.at[0, pl.ds(0, 3), rows]
        pending.append((cond, pltpu.make_async_copy(three, three, send_sem.at[len(pending)]).wait))

    def t_arrived(cond, i, xs, rows):
        arrived(cond, *t_at(i, xs, rows))

    x_others, y_others = [dev_x(v) for v in (xf, xp, xm)], [dev_y(v) for v in (yf, yp, ym)]
    end_cls = both(end, cls)

    def t_start():
        for rows in (TA, TR):
            region, sem = t_at(yi, x, rows)
            send(both(end_cls, g_own == 0), t_in.at[rows], region, sem, border)
            send(both(end_cls, g_own == 1), t_in.at[rows], region, sem, behind)
            when(own_near, pltpu.make_async_copy(t_in.at[rows], region, sem).start)

    def t_own(cond):
        t_arrived(cond, yi, x, TA)
        t_send(cond, yi, x, TA, x_others)
        t_arrived(cond, yi, x, TR)
        t_send(cond, yi, x, TR, y_others)
        t_send(cond, yi, x, TR, x_others)
        t_send(cond, yi, x, TA, y_others)

    def t_second(g):
        for xs in cols_of(g, yi):
            t_arrived(both(cls, xs != x), yi, xs, TA)
            t_send(both(cls, xs != x), yi, xs, TA, y_others)
        i = row_of(g, x)
        cond = jnp.logical_or(non, i != yi)
        t_arrived(cond, i, x, TR)
        t_send(cond, i, x, TR, x_others)

    def t_join(g):
        for i in (0, 1):
            for xs in cols_of(g, i):
                t_arrived(jnp.logical_or(non, yi != i), i, xs, TA)
                t_arrived(xs != x, i, xs, TR)
            n, k = (g, 2 * g) if i == 0 else (3 - g, 2 * (1 - g))
            tn[n, 0:TB, :] = tb[i, k, 0:TB, :]
            tn[n, TB:V, :] = tb[i, k + 1, 0:TB, :]

    t_start()
    l_first()
    t_own(own_near)
    l_own(0)
    l_own(1)
    l_relay_across(0, j1)
    send(mid, own_l(1 - ph, 1), l_at(1, vj), l_sem.at[1, vj], up)
    l_share(end, 0, j1)
    l_share(mid, 0, je)
    t_second(g_near)
    t_own(own_far)
    l_relay_across(0, j2)
    l_share(end, 1, j1)
    l_relay_across(1, j1)
    l_share(end, 0, j2)
    l_share(mid, 1, je)
    l_relay_across(1, j2)
    l_share(end, 0, j3)
    t_second(g_far)
    t_join(g_near)
    partner_j = [2 * s + 1 - core for s in range(4)]
    l_arrived(None, 0, vj)
    for j in partner_j:
        l_arrived(None, 0, j)

    def lay(pair):
        rows = lr[pair].reshape(2, W, W)
        lk[pair, :, :W] = rows[0]
        lk[pair, :, W:] = rows[1]

    def first_half(pair, k, n):
        half = lax.dot_general(tn[n], lr[pair].reshape(2 * W, W), NT, preferred_element_type=F32).astype(BF)
        h[:W, k * W:(k + 1) * W] = half[:, :W]
        h[W:, k * W:(k + 1) * W] = half[:, W:]

    def join_halves(pair, g):
        first_half(pair, 0, g)
        first_half(pair, 1, 3 - g)

    def first(g):
        join_halves(0, g)
        acc[...] = jnp.dot(lk[0], h[...], preferred_element_type=F32)

    A, B = pl.ds(0, 160), pl.ds(160, 160)

    def large(g, part):
        for slot, v in ((2, xf), (0, xp), (1, xm)):
            i = row_of(g, v)
            send(v % 2 == part, sb.at[i, v, B], rxb.at[slot, i], rxb_sem.at[slot, i], dev_x(v))
        xs = cols_of(g, 1 - yi)[part]
        send(cls, sb.at[1 - yi, xs, A], rya.at[2, xs], rya_sem.at[2, xs], dev_y(yf))
        xs = cols_of(g, ip)[part]
        send(non, sb.at[ip, xs, A], rya.at[0, xs], rya_sem.at[0, xs], dev_y(yp))
        xs = cols_of(g, im)[part]
        send(non, sb.at[im, xs, A], rya.at[1, xs], rya_sem.at[1, xs], dev_y(ym))

    def second(g):
        for part in (0, 1):
            rows = slice(part * SW, (part + 1) * SW)
            total = acc[rows, :] + jnp.dot(lk[1, rows, :], h[...], preferred_element_type=F32)
            for k, c in ((0, g), (1, 1 - g)):
                sb[k, 2 * c + part] = total[:, k * W:(k + 1) * W].astype(BF)
            large(g, part)

    lay(0)
    first(g_near)
    l_share(end, 1, j2)
    l_share(end, 1, j3)
    l_arrived(None, 1, vj)
    for j in partner_j:
        l_arrived(None, 1, j)

    @pl.when(end)
    def _():
        pl.semaphore_signal(line_sem, inc=1, device_id=border, device_id_type=MESH)

    lay(1)
    join_halves(1, g_near)
    second(g_near)


    def add(i, xs, rows, *others):
        total = sb[i, xs, rows, :].astype(F32)
        for other in others:
            total = total + other[...].astype(F32)
        return total

    def put(cond, i, xs, rows, *others):
        def work():
            sb[i, xs, rows, :] = add(i, xs, rows, *others).astype(BF)
        when(cond, work)

    def small(g):
        i = row_of(g, x)
        for slot in range(3):
            arrived(None, rxb.at[slot, i], rxb_sem.at[slot, i])
        put(None, i, x, B, rxb.at[0, i], rxb.at[1, i], rxb.at[2, i])
        send(both(cls, yi != i), sb.at[i, x, B], ryb.at[2], ryb_sem.at[2], dev_y(yf))
        send(both(non, ip == i), sb.at[i, x, B], ryb.at[0], ryb_sem.at[0], dev_y(yp))
        send(both(non, im == i), sb.at[i, x, B], ryb.at[1], ryb_sem.at[1], dev_y(ym))
        for xs in cols_of(g, yi):
            for slot in range(3):
                arrived(cls, rya.at[slot, xs], rya_sem.at[slot, xs])
            put(cls, yi, xs, A, rya.at[0, xs], rya.at[1, xs], rya.at[2, xs])
        for slot, v in ((2, xf), (0, xp), (1, xm)):
            send(both(cls, row_of(g, v) == yi), sb.at[yi, v, A], rxa.at[slot], rxa_sem.at[slot], dev_x(v))

    t_join(g_far)
    first(g_far)
    join_halves(1, g_far)
    second(g_far)
    small(g_near)
    pl.semaphore_wait(line_sem, 1)

    @pl.when(end)
    def _():
        pl.semaphore_signal(line_sem, inc=1, device_id=up, device_id_type=MESH)

    small(g_far)
    for slot in range(3):
        arrived(cls, ryb.at[slot], ryb_sem.at[slot])
        arrived(cls, rxa.at[slot], rxa_sem.at[slot])

    @pl.when(cls)
    def _():
        fin[0:160, :] = add(yi, x, A, rxa.at[0], rxa.at[1], rxa.at[2])
        fin[160:320, :] = add(yi, x, B, ryb.at[0], ryb.at[1], ryb.at[2])
        fin[320:, :] = jnp.zeros((64, W), F32)
        zs[...] = fin[...].T.astype(BF).reshape(8, LW, 384)

    away = z_owner != zh
    z_first = jnp.where((zl < 2) == away, 0, 3)
    z_step = jnp.where(z_first == 0, 1, -1)
    for o in range(4):
        for k in (0, 1):
            j = (z_first + o * z_step) * 2 + k
            send(both(cls, jnp.logical_or(away, j != vj)), zs.at[j], zr.at[zl], z_sem.at[zl],
                 dev(z_owner * 16 + y * 4 + x, j))
    when(both(cls, z_owner == zh), pltpu.make_async_copy(zs.at[vj], zr.at[zl], z_sem.at[zl]).start)
    for s in range(4):
        arrived(None, zr.at[s], z_sem.at[s])
    total = zr[0].astype(F32) + zr[1].astype(F32) + zr[2].astype(F32) + zr[3].astype(F32)
    for q in range(4):
        out[:, q * LB:(q + 1) * LB] = total[:LB, q * LW:q * LW + LB]

    assert len(pending) <= N_SEND, len(pending)
    for cond, wait in pending:
        when(cond, wait)


def shards(amplitudes, chol_vectors):
    dma = pltpu.SemaphoreType.DMA
    vmem = pltpu.VMEM
    turned = pl.pallas_call(
        kernel,
        out_shape=jax.ShapeDtypeStruct((LB, TB), F32),
        in_specs=[pl.BlockSpec(memory_space=pltpu.VMEM)] * 2,
        out_specs=pl.BlockSpec(memory_space=pltpu.VMEM),
        scratch_shapes=[
            vmem((TW, W), BF), vmem((8, LW, W), BF),
            vmem((2, 2, 8, LW, W), BF), vmem((2, W, 2 * W), BF),
            vmem((2, 4, TW, W), BF), vmem((4, W, W), BF), vmem((2 * W, 2 * W), BF),
            vmem((W, 2 * W), F32), vmem((2, 4, SW, W), BF),
            vmem((3, 2, 160, W), BF), vmem((3, 4, 160, W), BF), vmem((3, 160, W), BF), vmem((3, 160, W), BF),
            vmem((384, W), F32), vmem((8, LW, 384), BF), vmem((4, LW, 384), BF),
            dma((N_SEND,)), dma((2, 8)), dma((2, 4, 2)),
            dma((3, 2)), dma((3, 4)), dma((3,)), dma((3,)), dma((4,)),
            pltpu.SemaphoreType.REGULAR,
        ],
        compiler_params=pltpu.CompilerParams(
            collective_id=0, has_side_effects=True, vmem_limit_bytes=52 << 20),
        name="ladder",
    )(amplitudes, chol_vectors)
    return turned.T


def solution(mesh):
    placed = (P("chol", None), P("chol", "virt", None))
    return jax.shard_map(
        shards, mesh=mesh, in_specs=placed, out_specs=P("chol", "virt"), check_vma=False
    )
```

```python
import jax
import jax.numpy as jnp
from jax import lax
from jax.experimental import pallas as pl
from jax.experimental.pallas import tpu as pltpu
from jax.sharding import PartitionSpec as P

BF, F32 = jnp.bfloat16, jnp.float32
MESH = pl.DeviceIdType.MESH
NT = (((1,), (1,)), ((), ()))
V, W = 600, 640
TB, TW = 300, 304
LB, LW = 75, 80
SW = 320
N_SEND = 90


def kernel(t_raw, l_raw, out, t_in, l_in, lr, lk, tb, tn, h, acc, sb,
           rxb, rya, ryb, rxa, fin, zs, zr,
           send_sem, l_sem, t_sem, rxb_sem, rya_sem, ryb_sem, rxa_sem, z_sem, line_sem):
    ci, vj = lax.axis_index("chol"), lax.axis_index("virt")
    zh, y, x = ci // 16, (ci // 4) % 4, ci % 4
    zl, core = vj // 2, vj % 2
    xp, xf, xm = (x + 1) % 4, (x + 2) % 4, (x + 3) % 4
    yp, ym = (y + 1) % 4, (y + 3) % 4
    end = jnp.logical_or(zl == 0, zl == 3)
    mid = jnp.logical_not(end)
    cls = y % 2 == core
    non = jnp.logical_not(cls)
    nh = jnp.where(end, 1 - zh, zh)
    ph = zl // 2
    d2 = jnp.where(zl < 2, 2, -2)
    yi, ip, im = y // 2, yp // 2, ym // 2
    yf = (y + 2) % 4

    def row_of(g, xs):
        return (xs // 2 + g) % 2

    def cols_of(g, i):
        first_col = 2 * ((i + g) % 2)
        return first_col, first_col + 1

    def both(a, b):
        return jnp.logical_and(a, b)

    g_own = (x // 2 + yi) % 2
    g_near = jnp.where(end, 1, 0)
    g_far = 1 - g_near
    z_owner = (nh + g_own) % 2

    def dev(chol, virt):
        return {"chol": chol, "virt": virt}

    def dev_x(v):
        return dev(zh * 16 + y * 4 + v, vj)

    def dev_y(v):
        return dev(zh * 16 + v * 4 + x, vj)

    partner = dev(ci, vj + 1 - 2 * core)

    border = dev((1 - zh) * 16 + y * 4 + x, (3 - zl) * 2 + core)
    behind = dev((1 - zh) * 16 + y * 4 + x, (3 - zl) * 2 + core - d2)
    ahead = dev((1 - zh) * 16 + y * 4 + x, (3 - zl + d2 // 2) * 2 + core)
    up, down = dev(ci, (vj + d2) % 8), dev(ci, (vj - d2 + 8) % 8)

    opposite = dev(ci, (vj + 2 * d2 + 8) % 8)

    barrier = pltpu.get_barrier_semaphore()
    for there in (dev_x(xp), dev_x(xm), dev_x(xf), dev_y(yp), dev_y(ym), dev_y(yf), up, opposite, partner):
        pl.semaphore_signal(barrier, inc=1, device_id=there, device_id_type=MESH)

    @pl.when(end)
    def _():
        pl.semaphore_signal(barrier, inc=1, device_id=border, device_id_type=MESH)
        pl.semaphore_signal(barrier, inc=1, device_id=behind, device_id_type=MESH)

    @pl.when(mid)
    def _():
        pl.semaphore_signal(barrier, inc=1, device_id=down, device_id_type=MESH)
        pl.semaphore_signal(barrier, inc=1, device_id=ahead, device_id_type=MESH)

    t_in[...] = jnp.zeros_like(t_in)
    t_in[:TB, :V] = t_raw[...]
    l_in[:, LB - 3:, :] = jnp.zeros((8, LW - LB + 3, W), BF)
    l_in[:, :, V - 88:] = jnp.zeros((8, LW, W - V + 88), BF)
    l_in[:, :LB, :V] = l_raw[...]
    tn[:, V:, :] = jnp.zeros((4, W - V, W), BF)
    fin[SW:, :] = jnp.zeros((64, W), BF)
    pl.semaphore_wait(barrier, 11)

    pending = []

    def when(cond, work):
        if cond is None:
            work()
        else:
            pl.when(cond)(work)

    def send(cond, src, dst, sem, there):
        copy = pltpu.make_async_remote_copy(
            src_ref=src, dst_ref=dst, send_sem=send_sem.at[len(pending)], recv_sem=sem,
            device_id=there, device_id_type=MESH)
        pending.append((cond, copy.wait_send))
        when(cond, copy.start)

    def arrived(cond, region, sem):
        when(cond, pltpu.make_async_copy(region, region, sem).wait)

    def own_l(half, pair):
        return l_in.at[pl.ds(half * 4 + pair * 2, 2)]

    def l_at(pair, j):
        return lr.at[pair, :, j]

    j1, j2, j3 = (vj + d2 + 8) % 8, (vj + 2 * d2 + 8) % 8, (vj + 3 * d2 + 8) % 8
    je = (vj - d2 + 8) % 8

    def l_first():
        send(mid, own_l(1 - ph, 0), l_at(0, vj), l_sem.at[0, vj], up)
        for pair in (0, 1):
            send(mid, own_l(ph, pair), l_at(pair, vj), l_sem.at[pair, vj], down)
            send(end, own_l(ph, pair), l_at(pair, vj), l_sem.at[pair, vj], up)
            send(end, own_l(1 - ph, pair), l_at(pair, vj), l_sem.at[pair, vj], opposite)

    def l_own(pair):
        send(None, own_l(ph, pair), l_at(pair, vj), l_sem.at[pair, vj], partner)
        pltpu.make_async_copy(own_l(ph, pair), l_at(pair, vj), l_sem.at[pair, vj]).start()

    def l_arrived(cond, pair, j):
        arrived(cond, l_at(pair, j), l_sem.at[pair, j])

    def l_pass(cond, pair, j, there):
        send(cond, l_at(pair, j), l_at(pair, j), l_sem.at[pair, j], there)

    def l_relay_across(pair, j):
        l_arrived(mid, pair, j)
        l_pass(mid, pair, j, down)
        l_pass(mid, pair, j, partner)

    def l_share(cond, pair, j):
        l_arrived(cond, pair, j)
        l_pass(cond, pair, j, partner)

    TA, TR = pl.ds(0, 160), pl.ds(160, 144)
    own_near, own_far = both(cls, g_own == g_near), both(cls, g_own == g_far)

    def t_at(i, xs, rows):
        return tb.at[i, xs, rows], t_sem.at[i, xs, 0 if rows is TA else 1]

    def t_send(cond, i, xs, rows, theres):
        region, sem = t_at(i, xs, rows)
        copies = [pltpu.make_async_remote_copy(
            src_ref=region, dst_ref=region, send_sem=send_sem.at[len(pending)], recv_sem=sem,
            device_id=there, device_id_type=MESH) for there in theres]

        def work():
            for copy in copies:
                copy.start()

        when(cond, work)
        three = tb.at[0, pl.ds(0, 3), rows]
        pending.append((cond, pltpu.make_async_copy(three, three, send_sem.at[len(pending)]).wait))

    def t_arrived(cond, i, xs, rows):
        arrived(cond, *t_at(i, xs, rows))

    x_others, y_others = [dev_x(v) for v in (xf, xp, xm)], [dev_y(v) for v in (yf, yp, ym)]
    end_cls = both(end, cls)

    def t_start():
        for rows in (TA, TR):
            region, sem = t_at(yi, x, rows)
            send(both(end_cls, g_own == 0), t_in.at[rows], region, sem, border)
            send(both(end_cls, g_own == 1), t_in.at[rows], region, sem, behind)
            when(own_near, pltpu.make_async_copy(t_in.at[rows], region, sem).start)

    def t_own(cond):
        t_arrived(cond, yi, x, TA)
        t_send(cond, yi, x, TA, x_others)
        t_arrived(cond, yi, x, TR)
        t_send(cond, yi, x, TR, y_others)
        t_send(cond, yi, x, TR, x_others)
        t_send(cond, yi, x, TA, y_others)

    def t_second(g):
        for xs in cols_of(g, yi):
            t_arrived(both(cls, xs != x), yi, xs, TA)
            t_send(both(cls, xs != x), yi, xs, TA, y_others)
        i = row_of(g, x)
        cond = jnp.logical_or(non, i != yi)
        t_arrived(cond, i, x, TR)
        t_send(cond, i, x, TR, x_others)

    def t_join(g):
        for i in (0, 1):
            for xs in cols_of(g, i):
                t_arrived(jnp.logical_or(non, yi != i), i, xs, TA)
                t_arrived(xs != x, i, xs, TR)
            n, k = (g, 2 * g) if i == 0 else (3 - g, 2 * (1 - g))
            tn[n, 0:TB, :] = tb[i, k, 0:TB, :]
            tn[n, TB:V, :] = tb[i, k + 1, 0:TB, :]

    t_start()
    l_first()
    t_own(own_near)
    l_own(0)
    l_own(1)
    l_relay_across(0, j1)
    send(mid, own_l(1 - ph, 1), l_at(1, vj), l_sem.at[1, vj], up)
    l_share(end, 0, j1)
    l_share(mid, 0, je)
    t_second(g_near)
    t_own(own_far)
    l_relay_across(0, j2)
    l_share(end, 1, j1)
    l_relay_across(1, j1)
    l_share(end, 0, j2)
    l_share(mid, 1, je)
    l_relay_across(1, j2)
    l_share(end, 0, j3)
    t_second(g_far)
    t_join(g_near)
    partner_j = [2 * s + 1 - core for s in range(4)]
    l_arrived(None, 0, vj)
    for j in partner_j:
        l_arrived(None, 0, j)

    def lay(pair):
        rows = lr[pair].reshape(2, W, W)
        lk[pair, :, :W] = rows[0]
        lk[pair, :, W:] = rows[1]

    def first_half(pair, k, n):
        half = lax.dot_general(tn[n], lr[pair].reshape(2 * W, W), NT, preferred_element_type=F32).astype(BF)
        h[:W, k * W:(k + 1) * W] = half[:, :W]
        h[W:, k * W:(k + 1) * W] = half[:, W:]

    def join_halves(pair, g):
        first_half(pair, 0, g)
        first_half(pair, 1, 3 - g)

    def first(g):
        join_halves(0, g)
        acc[...] = jnp.dot(lk[0], h[...], preferred_element_type=F32)

    A, B = pl.ds(0, 160), pl.ds(160, 160)

    def large(g, part):
        for slot, v in ((2, xf), (0, xp), (1, xm)):
            i = row_of(g, v)
            send(v % 2 == part, sb.at[i, v, B], rxb.at[slot, i], rxb_sem.at[slot, i], dev_x(v))
        xs = cols_of(g, 1 - yi)[part]
        send(cls, sb.at[1 - yi, xs, A], rya.at[2, xs], rya_sem.at[2, xs], dev_y(yf))
        xs = cols_of(g, ip)[part]
        send(non, sb.at[ip, xs, A], rya.at[0, xs], rya_sem.at[0, xs], dev_y(yp))
        xs = cols_of(g, im)[part]
        send(non, sb.at[im, xs, A], rya.at[1, xs], rya_sem.at[1, xs], dev_y(ym))

    def second(g):
        for part in (0, 1):
            rows = slice(part * SW, (part + 1) * SW)
            total = acc[rows, :] + jnp.dot(lk[1, rows, :], h[...], preferred_element_type=F32)
            for k, c in ((0, g), (1, 1 - g)):
                sb[k, 2 * c + part] = total[:, k * W:(k + 1) * W].astype(BF)
            large(g, part)

    lay(0)
    first(g_near)
    l_share(end, 1, j2)
    l_share(end, 1, j3)
    l_arrived(None, 1, vj)
    for j in partner_j:
        l_arrived(None, 1, j)

    @pl.when(end)
    def _():
        pl.semaphore_signal(line_sem, inc=1, device_id=border, device_id_type=MESH)

    lay(1)
    join_halves(1, g_near)
    second(g_near)


    def add(i, xs, rows, *others):
        total = sb[i, xs, rows, :].astype(F32)
        for other in others:
            total = total + other[...].astype(F32)
        return total

    def put(cond, i, xs, rows, *others):
        def work():
            sb[i, xs, rows, :] = add(i, xs, rows, *others).astype(BF)
        when(cond, work)

    def small(g):
        i = row_of(g, x)
        for slot in range(3):
            arrived(None, rxb.at[slot, i], rxb_sem.at[slot, i])
        put(None, i, x, B, rxb.at[0, i], rxb.at[1, i], rxb.at[2, i])
        send(both(cls, yi != i), sb.at[i, x, B], ryb.at[2], ryb_sem.at[2], dev_y(yf))
        send(both(non, ip == i), sb.at[i, x, B], ryb.at[0], ryb_sem.at[0], dev_y(yp))
        send(both(non, im == i), sb.at[i, x, B], ryb.at[1], ryb_sem.at[1], dev_y(ym))
        for xs in cols_of(g, yi):
            for slot in range(3):
                arrived(cls, rya.at[slot, xs], rya_sem.at[slot, xs])
            put(cls, yi, xs, A, rya.at[0, xs], rya.at[1, xs], rya.at[2, xs])
        for slot, v in ((2, xf), (0, xp), (1, xm)):
            send(both(cls, row_of(g, v) == yi), sb.at[yi, v, A], rxa.at[slot], rxa_sem.at[slot], dev_x(v))

    t_join(g_far)
    first(g_far)
    join_halves(1, g_far)
    second(g_far)
    small(g_near)
    pl.semaphore_wait(line_sem, 1)

    @pl.when(end)
    def _():
        pl.semaphore_signal(line_sem, inc=1, device_id=up, device_id_type=MESH)

    small(g_far)
    for slot in range(3):
        arrived(cls, ryb.at[slot], ryb_sem.at[slot])
        arrived(cls, rxa.at[slot], rxa_sem.at[slot])

    @pl.when(cls)
    def _():
        fin[0:160, :] = add(yi, x, A, rxa.at[0], rxa.at[1], rxa.at[2]).astype(BF)
        fin[160:320, :] = add(yi, x, B, ryb.at[0], ryb.at[1], ryb.at[2]).astype(BF)
        zs[...] = fin[...].T.reshape(8, LW, 384)

    away = z_owner != zh
    z_first = jnp.where((zl < 2) == away, 0, 3)
    z_step = jnp.where(z_first == 0, 1, -1)
    for o in range(4):
        for k in (0, 1):
            j = (z_first + o * z_step) * 2 + k
            send(both(cls, jnp.logical_or(away, j != vj)), zs.at[j], zr.at[zl], z_sem.at[zl],
                 dev(z_owner * 16 + y * 4 + x, j))
    when(both(cls, z_owner == zh), pltpu.make_async_copy(zs.at[vj], zr.at[zl], z_sem.at[zl]).start)
    for s in range(4):
        arrived(None, zr.at[s], z_sem.at[s])
    total = zr[0].astype(F32) + zr[1].astype(F32) + zr[2].astype(F32) + zr[3].astype(F32)
    for q in range(4):
        out[:, q * LB:(q + 1) * LB] = total[:LB, q * LW:q * LW + LB]

    assert len(pending) <= N_SEND, len(pending)
    for cond, wait in pending:
        when(cond, wait)


def shards(amplitudes, chol_vectors):
    dma = pltpu.SemaphoreType.DMA
    vmem = pltpu.VMEM
    turned = pl.pallas_call(
        kernel,
        out_shape=jax.ShapeDtypeStruct((LB, TB), F32),
        in_specs=[pl.BlockSpec(memory_space=pltpu.VMEM)] * 2,
        out_specs=pl.BlockSpec(memory_space=pltpu.VMEM),
        scratch_shapes=[
            vmem((TW, W), BF), vmem((8, LW, W), BF),
            vmem((2, 2, 8, LW, W), BF), vmem((2, W, 2 * W), BF),
            vmem((2, 4, TW, W), BF), vmem((4, W, W), BF), vmem((2 * W, 2 * W), BF),
            vmem((W, 2 * W), F32), vmem((2, 4, SW, W), BF),
            vmem((3, 2, 160, W), BF), vmem((3, 4, 160, W), BF), vmem((3, 160, W), BF), vmem((3, 160, W), BF),
            vmem((384, W), BF), vmem((8, LW, 384), BF), vmem((4, LW, 384), BF),
            dma((N_SEND,)), dma((2, 8)), dma((2, 4, 2)),
            dma((3, 2)), dma((3, 4)), dma((3,)), dma((3,)), dma((4,)),
            pltpu.SemaphoreType.REGULAR,
        ],
        compiler_params=pltpu.CompilerParams(
            collective_id=0, has_side_effects=True, vmem_limit_bytes=52 << 20),
        name="ladder",
    )(amplitudes, chol_vectors)
    return turned.T


def solution(mesh):
    placed = (P("chol", None), P("chol", "virt", None))
    return jax.shard_map(
        shards, mesh=mesh, in_specs=placed, out_specs=P("chol", "virt"), check_vma=False
    )
```
